8 devices in a mesh: rep: 1 (over z), dp: 8 (over x, y, core).
Axes of the slice: x: 2, y: 2, z: 1, core: 2. Of those that a mesh axis runs over, the one named last changes fastest.
Arguments:
- a: bfloat16 [8, 4, 4096, 1280], P(('rep', 'dp'))
- g: bfloat16 [8, 4, 4096, 3072], P(('rep', 'dp'))
Outputs:
- output: bfloat16 [4, 1280, 3072], P('rep')
All inputs are finite; a program needn't handle non-finite values.
Results may differ from the reference program's by a relative error of at most 0.012.
Values are sent between devices in bfloat16 or wider.
A program may use at most 2 GiB of HBM per device.

```python
import jax
import jax.numpy as jnp
from jax import lax

DEVICES = 8
MATRICES = 4
TOKENS = 4096
D = 1280
FF = 3072


def setup_inputs(seed: int = 0, part: int = 0) -> dict:
    ka, kg, ks = (jax.random.fold_in(k, part) for k in jax.random.split(jax.random.key(seed), 3))
    size = 2.0 ** jax.random.uniform(ks, (DEVICES, MATRICES, 1, 1), jnp.float32, -1.0, 1.0)
    a = jax.random.normal(ka, (DEVICES, MATRICES, TOKENS, D), jnp.float32)
    g = size * jax.random.normal(kg, (DEVICES, MATRICES, TOKENS, FF), jnp.float32) * (DEVICES * TOKENS) ** -0.5
    return {"a": a.astype(jnp.bfloat16), "g": g.astype(jnp.bfloat16)}


def reference(a, g):
    def take(so_far, one):
        return so_far + jnp.einsum("ntd,ntf->ndf", *one, preferred_element_type=jnp.float32), None

    return lax.scan(take, jnp.zeros((MATRICES, D, FF), jnp.float32), (a, g))[0].astype(jnp.bfloat16)
```

```python
import functools

import jax
import jax.numpy as jnp
from jax import lax
from jax.experimental import pallas as pl
from jax.experimental.pallas import tpu as pltpu
from jax.sharding import PartitionSpec as P

MESH = pl.DeviceIdType.MESH
MATS, TOKENS, D, FF = 4, 4096, 1280, 3072
HALF = D // 2
TN = 512
PANELS = FF // TN
ROUNDS = MATS * PANELS // 4
SLOTS = ROUNDS * 4
RB = 80
F32, BF16 = jnp.float32, jnp.bfloat16


def dev(i):
    return {"rep": 0, "dp": i}


def place():
    me = lax.axis_index("dp")
    x, y, core = me // 4, (me // 2) % 2, me % 2
    xn = (1 - x) * 4 + y * 2 + core
    yn = x * 4 + (1 - y) * 2 + core
    partner = x * 4 + y * 2 + (1 - core)
    first = jnp.where(core == 0, xn, yn)
    second = jnp.where(core == 0, yn, xn)
    return x, y, core, first, second, partner


def remote(src, dst, ssem, rsem, to):
    return pltpu.make_async_remote_copy(
        src_ref=src, dst_ref=dst, send_sem=ssem, recv_sem=rsem, device_id=dev(to), device_id_type=MESH
    )


def meet(*others):
    barrier = pltpu.get_barrier_semaphore()
    for other in others:
        pl.semaphore_signal(barrier, inc=1, device_id=dev(other), device_id_type=MESH)
    pl.semaphore_wait(barrier, len(others))


def reduce_kernel(
    a, g, own, abuf, gbuf, acc, dsend, drecv, sbuf, rbuf, fbuf, asem, gsem, dssem, drsem, ssem, rsem, fsem
):
    x, y, core, first, second, partner = place()

    def aload(n, half):
        cols = pl.ds(pl.multiple_of(half * HALF, 128), HALF)
        return pltpu.make_async_copy(a.at[n, :, cols], abuf.at[n % 2, half], asem.at[n % 2, half])

    def where_is(t):
        r, i = t // 4, t % 4
        jx = jnp.where(i < 2, 1 - x, x)
        jy = jnp.where(i % 2 == 0, 1 - y, y)
        q = 4 * r + 2 * jx + jy
        return q // PANELS, q % PANELS

    def gload(t):
        n, p = where_is(t)
        cols = pl.ds(pl.multiple_of(p * TN, 128), TN)
        return pltpu.make_async_copy(g.at[n, :, cols], gbuf.at[t % 2], gsem.at[t % 2])

    def partner_copy(t):
        return remote(dsend.at[t % 2], drecv.at[t % 2], dssem.at[t % 2], drsem.at[t % 2], partner)

    def hop(r, kind, to):
        rp = r % 2
        return remote(sbuf.at[rp, kind], rbuf.at[rp, kind], ssem.at[rp, kind], rsem.at[rp, kind], to)

    def finished(r):
        return pltpu.make_async_copy(fbuf.at[r % 2], own.at[r], fsem.at[r % 2])

    def rows(fn):
        def one(b, _):
            fn(pl.ds(pl.multiple_of(b * RB, 16), RB))
            return 0

        lax.fori_loop(0, HALF // RB, one, 0)

    def finish(r):
        rp = r % 2
        hop(r, 1, first).wait_recv()
        hop(r, 2, second).wait_recv()

        @pl.when(r >= 2)
        def _():
            finished(r - 2).wait()

        def add(s):
            total = acc[3, s, :] + rbuf[rp, 1, s, :].astype(F32) + rbuf[rp, 2, s, :].astype(F32)
            fbuf[rp, s, :] = total.astype(BF16)

        rows(add)
        finished(r).start()

    aload(0, 1 - core).start()
    gload(0).start()
    aload(0, core).start()
    aload(1, 1 - core).start()
    aload(1, core).start()
    meet(first, second, partner)

    def dot(n, half, t):
        return lax.dot_general(
            abuf[n % 2, half], gbuf[t % 2], (((0,), (0,)), ((), ())), preferred_element_type=F32
        )

    def slot(t, _):
        r, i = t // 4, t % 4
        rp = r % 2
        n, _p = where_is(t)

        @pl.when(t == 0)
        def _():
            aload(0, 1 - core).wait()

        for rr, (wait_n, start_n) in {1: (1, None), 2: (None, 2), 3: (2, 3), 4: (3, None)}.items():

            @pl.when(t == 4 * rr)
            def _():
                for half in (0, 1):
                    if wait_n is not None:
                        aload(wait_n, half).wait()
                    if start_n is not None:
                        aload(start_n, half).start()

        gload(t).wait()

        @pl.when(t + 1 < SLOTS)
        def _():
            gload(t + 1).start()

        @pl.when(t >= 2)
        def _():
            partner_copy(t - 2).wait_send()

        dsend[t % 2] = dot(n, 1 - core, t).astype(BF16)
        partner_copy(t).start()

        @pl.when(t == 0)
        def _():
            aload(0, core).wait()

        acc[i] = dot(n, core, t)
        partner_copy(t).wait_recv()

        def add(s):
            acc[i, s, :] = acc[i, s, :] + drecv[t % 2, s, :].astype(F32)

        rows(add)

        def ready(kind):
            @pl.when(r >= 2)
            def _():
                hop(r - 2, kind, first).wait_send()

        def send_raw(kind):
            ready(kind)

            def put(s):
                sbuf[rp, kind, s, :] = acc[i, s, :].astype(BF16)

            rows(put)
            hop(r, kind, first).start()

        @pl.when(i == 0)
        def _():
            send_raw(0)

        @pl.when((i == 1) & (r >= 1))
        def _():
            finish(r - 1)

        @pl.when(i == 1 + core)
        def _():
            send_raw(1)

        @pl.when(i == 2)
        def _():
            hop(r, 0, first).wait_recv()
            ready(2)

            def put(s):
                sbuf[rp, 2, s, :] = (acc[2 - core, s, :] + rbuf[rp, 0, s, :].astype(F32)).astype(BF16)

            rows(put)
            hop(r, 2, second).start()

        return 0

    lax.fori_loop(0, SLOTS, slot, 0)
    finish(ROUNDS - 1)
    for t in (SLOTS - 2, SLOTS - 1):
        partner_copy(t).wait_send()
    for r in (ROUNDS - 2, ROUNDS - 1):
        for kind in range(3):
            hop(r, kind, first).wait_send()
        finished(r).wait()


def gather_kernel(own, out, lsem, ssem, rsem, dssem, drsem):
    x, y, core, first, second, partner = place()
    chip = 2 * x + y
    first_chip = jnp.where(core == 0, 2 * (1 - x) + y, 2 * x + 1 - y)
    second_chip = jnp.where(core == 0, 2 * x + 1 - y, 2 * (1 - x) + y)
    diagonal = 3 - chip

    def part(r, c, half):
        q = 4 * r + c
        return out.at[
            q // PANELS,
            pl.ds(pl.multiple_of(half * HALF, 16), HALF),
            pl.ds(pl.multiple_of((q % PANELS) * TN, 128), TN),
        ]

    def local(r):
        return pltpu.make_async_copy(own.at[r], part(r, chip, core), lsem.at[r])

    def to_first(r):
        return remote(own.at[r], part(r, chip, core), ssem.at[r, 0], rsem.at[r, 0], first)

    def to_second(r):
        return remote(own.at[r], part(r, chip, core), ssem.at[r, 1], rsem.at[r, 1], second)

    def forward(r):
        return remote(part(r, second_chip, core), part(r, second_chip, core), ssem.at[r, 2], rsem.at[r, 2], first)

    def across_own(r):
        return remote(own.at[r], part(r, chip, core), dssem.at[r, 0], drsem.at[r, 0], partner)

    def across(r, k, c):
        return remote(part(r, c, core), part(r, c, core), dssem.at[r, k], drsem.at[r, k], partner)

    meet(first, second, partner)

    def begin(r, _):
        to_first(r).start()
        to_second(r).start()
        across_own(r).start()
        local(r).start()
        return 0

    lax.fori_loop(0, ROUNDS, begin, 0)

    def middle(r, _):
        to_second(r).wait_recv()
        forward(r).start()
        across(r, 1, second_chip).start()
        to_first(r).wait_recv()
        across(r, 2, first_chip).start()
        return 0

    lax.fori_loop(0, ROUNDS, middle, 0)

    def last(r, _):
        forward(r).wait_recv()
        across(r, 3, diagonal).start()
        return 0

    lax.fori_loop(0, ROUNDS, last, 0)

    def drain(r, _):
        local(r).wait()
        to_first(r).wait_send()
        to_second(r).wait_send()
        forward(r).wait_send()
        for k in range(4):
            across(r, k, diagonal).wait()
        return 0

    lax.fori_loop(0, ROUNDS, drain, 0)


def write_kernel(held, out, sem):
    copies = [pltpu.make_async_copy(held.at[n], out.at[n], sem.at[n]) for n in range(MATS)]
    for copy in copies:
        copy.start()
    for copy in copies:
        copy.wait()


def solution(mesh):
    any_space = pl.BlockSpec(memory_space=pl.ANY)
    hbm = pl.BlockSpec(memory_space=pltpu.HBM)
    vmem = pl.BlockSpec(memory_space=pltpu.VMEM)
    dma = pltpu.SemaphoreType.DMA

    def body(a, g):
        own = pl.pallas_call(
            reduce_kernel,
            out_shape=pltpu.HBM((ROUNDS, HALF, TN), BF16),
            in_specs=[any_space] * 2,
            out_specs=hbm,
            scratch_shapes=[
                pltpu.VMEM((2, 2, TOKENS, HALF), BF16),
                pltpu.VMEM((2, TOKENS, TN), BF16),
                pltpu.VMEM((4, HALF, TN), F32),
                pltpu.VMEM((2, HALF, TN), BF16),
                pltpu.VMEM((2, HALF, TN), BF16),
                pltpu.VMEM((2, 3, HALF, TN), BF16),
                pltpu.VMEM((2, 3, HALF, TN), BF16),
                pltpu.VMEM((2, HALF, TN), BF16),
                dma((2, 2)),
                dma((2,)),
                dma((2,)),
                dma((2,)),
                dma((2, 3)),
                dma((2, 3)),
                dma((2,)),
            ],
            compiler_params=pltpu.CompilerParams(
                collective_id=0, has_side_effects=True, vmem_limit_bytes=60 * 2**20
            ),
            name="reduce_scatter",
        )(a[0], g[0])
        held = pl.pallas_call(
            gather_kernel,
            out_shape=pltpu.VMEM((MATS, D, FF), BF16),
            in_specs=[hbm],
            out_specs=vmem,
            scratch_shapes=[
                dma((ROUNDS,)),
                dma((ROUNDS, 3)),
                dma((ROUNDS, 3)),
                dma((ROUNDS, 4)),
                dma((ROUNDS, 4)),
            ],
            compiler_params=pltpu.CompilerParams(
                collective_id=1, has_side_effects=True, vmem_limit_bytes=16 * 2**20
            ),
            name="all_gather",
        )(own)
        return pl.pallas_call(
            write_kernel,
            out_shape=jax.ShapeDtypeStruct((MATS, D, FF), BF16),
            in_specs=[vmem],
            out_specs=any_space,
            scratch_shapes=[dma((MATS,))],
            compiler_params=pltpu.CompilerParams(vmem_limit_bytes=16 * 2**20),
            name="write_out",
        )(held)

    return jax.shard_map(
        body, mesh=mesh, in_specs=P(("rep", "dp")), out_specs=P("rep"), check_vma=False
    )
```

```python
import functools

import jax
import jax.numpy as jnp
from jax import lax
from jax.experimental import pallas as pl
from jax.experimental.pallas import tpu as pltpu
from jax.sharding import PartitionSpec as P

MESH = pl.DeviceIdType.MESH
MATS, TOKENS, D, FF = 4, 4096, 1280, 3072
HALF = D // 2
TN = 512
PANELS = FF // TN
ROUNDS = MATS * PANELS // 4
SLOTS = ROUNDS * 4
RB = 80
F32, BF16 = jnp.float32, jnp.bfloat16
S_AT = (3, 7, 11, 15, 19, 22)
O_AT = (6, 10, 14, 18, 22, 25)
AG_AT = (
    *((0, 0, 8), (0, 1, 11), (0, 2, 14), (0, 3, 14), (0, 4, 24), (1, 0, 15), (1, 1, 18)),
    *((2, 0, 24), (3, 0, 24), (4, 0, 24), (1, 2, 24), (2, 1, 24), (3, 1, 24), (4, 1, 24), (1, 3, 24)),
    *((5, 0, 25), (5, 1, 25), (2, 2, 26), (2, 3, 26), (3, 2, 26), (3, 3, 26), (4, 2, 26), (4, 3, 26), (5, 2, 26), (5, 3, 26)),
    *((1, 4, 27), (2, 4, 27), (3, 4, 27), (4, 4, 27), (5, 4, 27)),
)


def dev(i):
    return {"rep": 0, "dp": i}


def place():
    me = lax.axis_index("dp")
    x, y, core = me // 4, (me // 2) % 2, me % 2
    xn = (1 - x) * 4 + y * 2 + core
    yn = x * 4 + (1 - y) * 2 + core
    partner = x * 4 + y * 2 + (1 - core)
    first = jnp.where(core == 0, xn, yn)
    second = jnp.where(core == 0, yn, xn)
    return x, y, core, first, second, partner


def remote(src, dst, ssem, rsem, to):
    return pltpu.make_async_remote_copy(
        src_ref=src, dst_ref=dst, send_sem=ssem, recv_sem=rsem, device_id=dev(to), device_id_type=MESH
    )


def meet(*others):
    barrier = pltpu.get_barrier_semaphore()
    for other in others:
        pl.semaphore_signal(barrier, inc=1, device_id=dev(other), device_id_type=MESH)
    pl.semaphore_wait(barrier, len(others))


def chips(x, y, core):
    xc, yc = 2 * (1 - x) + y, 2 * x + 1 - y
    return 2 * x + y, jnp.where(core == 0, xc, yc), jnp.where(core == 0, yc, xc)


class Gather:
    def __init__(self, sems, part, own):
        self.ssem, self.rsem, self.dssem, self.drsem = sems
        self.part, self.own = part, own
        self.x, self.y, self.core, self.first, self.second, self.partner = place()
        self.chip, self.first_chip, self.second_chip = chips(self.x, self.y, self.core)

    def chip_copy(self, src, c, r, kind, to):
        return remote(src, self.part(r, c, self.core), self.ssem.at[r, kind], self.rsem.at[r, kind], to)

    def to_first(self, r):
        return self.chip_copy(self.own(r), self.chip, r, 0, self.first)

    def to_second(self, r):
        return self.chip_copy(self.own(r), self.chip, r, 1, self.second)

    def forward(self, r):
        return self.chip_copy(self.part(r, self.second_chip, self.core), self.second_chip, r, 2, self.first)

    def across_own(self, r):
        return remote(
            self.own(r), self.part(r, self.chip, self.core), self.dssem.at[r, 0], self.drsem.at[r, 0], self.partner
        )

    def across(self, r, k, c):
        part = self.part(r, c, self.core)
        return remote(part, part, self.dssem.at[r, k], self.drsem.at[r, k], self.partner)

    def drain(self, r):
        self.to_first(r).wait_send()
        self.to_second(r).wait_send()
        self.forward(r).wait_send()
        for k in range(4):
            self.across(r, k, self.chip).wait()


def sum_kernel(
    a,
    g,
    out,
    abuf,
    gbuf,
    acc,
    dsend,
    drecv,
    sbuf,
    rbuf_d,
    rbuf_f,
    rbuf_s,
    asem,
    gsem,
    dssem,
    drsem,
    ssem,
    rsem,
    *gsems,
):
    x, y, core, first, second, partner = place()
    chip, first_chip, second_chip = chips(x, y, core)

    def part(r, c, half):
        q = 4 * r + c
        return out.at[
            q // PANELS,
            pl.ds(pl.multiple_of(half * HALF, 16), HALF),
            pl.ds(pl.multiple_of((q % PANELS) * TN, 128), TN),
        ]

    gather = Gather(gsems, part, lambda r: part(r, chip, core))

    def where_is(t):
        r, i = t // 4, t % 4
        jx = jnp.where(i < 2, 1 - x, x)
        jy = jnp.where(i % 2 == 0, 1 - y, y)
        q = 4 * r + 2 * jx + jy
        return q // PANELS, q % PANELS

    def aload(t, mine):
        n, _ = where_is(t)
        half = core if mine else 1 - core
        cols = pl.ds(pl.multiple_of(half * HALF, 128), HALF)
        return pltpu.make_async_copy(a.at[n, :, cols], abuf.at[int(mine)], asem.at[int(mine)])

    def gload(t):
        n, p = where_is(t)
        cols = pl.ds(pl.multiple_of(p * TN, 128), TN)
        return pltpu.make_async_copy(g.at[n, :, cols], gbuf.at[t % 2], gsem.at[t % 2])

    def partner_copy(t):
        return remote(dsend, drecv.at[t % 2], dssem, drsem.at[t % 2], partner)

    def hop(r, kind):
        depth, rbuf = ((2, rbuf_d), (3, rbuf_f), (3, rbuf_s))[kind]
        return remote(
            sbuf.at[r % 2, kind],
            rbuf.at[r % depth],
            ssem.at[r % 2, kind],
            rsem.at[r % depth, kind],
            second if kind == 2 else first,
        )

    def rows(fn):
        def one(b, _):
            fn(pl.ds(pl.multiple_of(b * RB, 16), RB))
            return 0

        lax.fori_loop(0, HALF // RB, one, 0)

    def ready(r, kind):
        @pl.when(r >= 2)
        def _():
            hop(r - 2, kind).wait_send()

    def pass_on(r):
        hop(r, 0).wait_recv()
        if r >= 2:
            hop(r - 2, 2).wait_send()

        def put(s):
            sbuf[r % 2, 2, s, :] = (acc[1, s, :] + rbuf_d[r % 2, s, :].astype(F32)).astype(BF16)

        rows(put)
        hop(r, 2).start()

    def finish(r):
        hop(r, 1).wait_recv()
        hop(r, 2).wait_recv()
        done = part(r, chip, core)

        def add(s):
            total = acc[2, s, :] + rbuf_f[r % 3, s, :].astype(F32) + rbuf_s[r % 3, s, :].astype(F32)
            done[s, :] = total.astype(BF16)

        rows(add)

    def spread(r, kind):
        if kind == 0:
            gather.to_first(r).start()
            gather.across_own(r).start()
        elif kind == 1:
            gather.to_second(r).start()
        elif kind == 2:
            gather.to_second(r).wait_recv()
            gather.forward(r).start()
            gather.across(r, 1, second_chip).start()
        elif kind == 3:
            gather.to_first(r).wait_recv()
            gather.across(r, 2, first_chip).start()
        else:
            gather.forward(r).wait_recv()
            gather.across(r, 3, 3 - chip).start()

    actions = [(t, functools.partial(finish, r)) for r, t in enumerate(O_AT)]
    actions += [(t, functools.partial(pass_on, r)) for r, t in enumerate(S_AT)]
    actions += [(t, functools.partial(spread, r, kind)) for r, kind, t in AG_AT]
    actions.sort(key=lambda action: action[0])

    aload(0, False).start()
    gload(0).start()
    aload(0, True).start()
    meet(first, second, partner)

    def dot(mine, t):
        return lax.dot_general(
            abuf[int(mine)], gbuf[t % 2], (((0,), (0,)), ((), ())), preferred_element_type=F32
        )

    def slot(t, _):
        r, i = t // 4, t % 4
        rp = r % 2
        aload(t, False).wait()
        gload(t).wait()

        @pl.when(t + 1 < SLOTS)
        def _():
            gload(t + 1).start()

        @pl.when(t >= 1)
        def _():
            partner_copy(t - 1).wait_send()

        dsend[...] = dot(False, t).astype(BF16)
        partner_copy(t).start()

        @pl.when(t + 1 < SLOTS)
        def _():
            aload(t + 1, False).start()

        aload(t, True).wait()
        kept = jnp.where(i == 3, 2, jnp.where(i == 2 - core, 1, 0))
        acc[kept] = dot(True, t)

        @pl.when(t + 1 < SLOTS)
        def _():
            aload(t + 1, True).start()

        partner_copy(t).wait_recv()

        def add(s):
            acc[kept, s, :] = acc[kept, s, :] + drecv[t % 2, s, :].astype(F32)

        rows(add)

        def send_raw(kind):
            ready(r, kind)

            def put(s):
                sbuf[rp, kind, s, :] = acc[0, s, :].astype(BF16)

            rows(put)
            hop(r, kind).start()

        @pl.when(i == 0)
        def _():
            send_raw(0)

        @pl.when(i == 1 + core)
        def _():
            send_raw(1)

        for at, act in actions:
            if at < SLOTS:
                pl.when(t == at)(act)

        return 0

    lax.fori_loop(0, SLOTS, slot, 0)
    for at, act in actions:
        if at >= SLOTS:
            act()
    partner_copy(SLOTS - 1).wait_send()
    for r in (ROUNDS - 2, ROUNDS - 1):
        for kind in range(3):
            hop(r, kind).wait_send()

    def drain(r, _):
        gather.drain(r)
        return 0

    lax.fori_loop(0, ROUNDS, drain, 0)


def write_kernel(held, out, sem):
    copies = [pltpu.make_async_copy(held.at[n], out.at[n], sem.at[n]) for n in range(MATS)]
    for copy in copies:
        copy.start()
    for copy in copies:
        copy.wait()


def solution(mesh):
    any_space = pl.BlockSpec(memory_space=pl.ANY)
    vmem = pl.BlockSpec(memory_space=pltpu.VMEM)
    dma = pltpu.SemaphoreType.DMA

    def body(a, g):
        held = pl.pallas_call(
            sum_kernel,
            out_shape=pltpu.VMEM((MATS, D, FF), BF16),
            in_specs=[any_space] * 2,
            out_specs=vmem,
            scratch_shapes=[
                pltpu.VMEM((2, TOKENS, HALF), BF16),
                pltpu.VMEM((2, TOKENS, TN), BF16),
                pltpu.VMEM((3, HALF, TN), F32),
                pltpu.VMEM((HALF, TN), BF16),
                pltpu.VMEM((2, HALF, TN), BF16),
                pltpu.VMEM((2, 3, HALF, TN), BF16),
                pltpu.VMEM((2, HALF, TN), BF16),
                pltpu.VMEM((3, HALF, TN), BF16),
                pltpu.VMEM((3, HALF, TN), BF16),
                dma((2,)),
                dma((2,)),
                dma,
                dma((2,)),
                dma((2, 3)),
                dma((3, 3)),
                dma((ROUNDS, 3)),
                dma((ROUNDS, 3)),
                dma((ROUNDS, 4)),
                dma((ROUNDS, 4)),
            ],
            compiler_params=pltpu.CompilerParams(
                collective_id=0, has_side_effects=True, vmem_limit_bytes=35_400_000
            ),
            name="sum_and_share",
        )(a[0], g[0])
        return pl.pallas_call(
            write_kernel,
            out_shape=jax.ShapeDtypeStruct((MATS, D, FF), BF16),
            in_specs=[vmem],
            out_specs=any_space,
            scratch_shapes=[dma((MATS,))],
            compiler_params=pltpu.CompilerParams(vmem_limit_bytes=16 * 2**20),
            name="write_out",
        )(held)

    return jax.shard_map(
        body, mesh=mesh, in_specs=P(("rep", "dp")), out_specs=P("rep"), check_vma=False
    )
```

```python
import functools

import jax
import jax.numpy as jnp
from jax import lax
from jax.experimental import pallas as pl
from jax.experimental.pallas import tpu as pltpu
from jax.sharding import PartitionSpec as P

MESH = pl.DeviceIdType.MESH
MATS, TOKENS, D, FF = 4, 4096, 1280, 3072
HALF = D // 2
TN = 512
PANELS = FF // TN
ROUNDS = MATS * PANELS // 4
SLOTS = ROUNDS * 4
RB = 80
F32, BF16 = jnp.float32, jnp.bfloat16
TH = TN // 2
BLOCKS = tuple((rs, cs) for cs in ((0, TH), (TH, TH)) for rs in ((0, 256), (256, HALF - 256)))
S_AT = ((1, 2), (6, 7), (10, 11), (14, 15), (18, 19), (22, 22))
O_AT = (4.5, 10, 14, 18, 22, 25)
AG_AT = (
    *((0, 0, 4.5), (0, 1, 5), (0, 2, 10), (0, 3, 10), (1, 0, 12), (1, 1, 16), (2, 0, 19), (2, 1, 21)),
    *((3, 0, 23), (3, 1, 24), (4, 0, 24), (4, 1, 24), (0, 4, 24), (5, 0, 25), (5, 1, 25)),
    *((r, kind, 26) for r in range(1, 6) for kind in (2, 3)),
    *((r, 4, 27) for r in range(1, 6)),
)


def dev(i):
    return {"rep": 0, "dp": i}


def place():
    me = lax.axis_index("dp")
    x, y, core = me // 4, (me // 2) % 2, me % 2
    xn = (1 - x) * 4 + y * 2 + core
    yn = x * 4 + (1 - y) * 2 + core
    partner = x * 4 + y * 2 + (1 - core)
    first = jnp.where(core == 0, xn, yn)
    second = jnp.where(core == 0, yn, xn)
    return x, y, core, first, second, partner


def remote(src, dst, ssem, rsem, to):
    return pltpu.make_async_remote_copy(
        src_ref=src, dst_ref=dst, send_sem=ssem, recv_sem=rsem, device_id=dev(to), device_id_type=MESH
    )


def greet(*others):
    for other in others:
        pl.semaphore_signal(pltpu.get_barrier_semaphore(), inc=1, device_id=dev(other), device_id_type=MESH)


def chips(x, y, core):
    xc, yc = 2 * (1 - x) + y, 2 * x + 1 - y
    return 2 * x + y, jnp.where(core == 0, xc, yc), jnp.where(core == 0, yc, xc)


class Gather:
    def __init__(self, sems, part, own):
        self.ssem, self.rsem, self.dssem, self.drsem = sems
        self.part, self.own = part, own
        self.x, self.y, self.core, self.first, self.second, self.partner = place()
        self.chip, self.first_chip, self.second_chip = chips(self.x, self.y, self.core)

    def chip_copy(self, src, c, r, kind, to):
        return remote(src, self.part(r, c, self.core), self.ssem.at[r, kind], self.rsem.at[r, kind], to)

    def to_first(self, r):
        return self.chip_copy(self.own(r), self.chip, r, 0, self.first)

    def to_second(self, r):
        return self.chip_copy(self.own(r), self.chip, r, 1, self.second)

    def forward(self, r):
        return self.chip_copy(self.part(r, self.second_chip, self.core), self.second_chip, r, 2, self.first)

    def across_own(self, r):
        return remote(
            self.own(r), self.part(r, self.chip, self.core), self.dssem.at[r, 0], self.drsem.at[r, 0], self.partner
        )

    def across(self, r, k, c):
        part = self.part(r, c, self.core)
        return remote(part, part, self.dssem.at[r, k], self.drsem.at[r, k], self.partner)

    def drain(self, r):
        self.to_first(r).wait_send()
        self.to_second(r).wait_send()
        self.forward(r).wait_send()
        for k in range(4):
            self.across(r, k, self.chip).wait()


def panel(r, jx, jy):
    return 4 * r + 2 * ((jx + jy) % 2) + jx


def sum_kernel(
    a,
    g,
    out,
    abuf,
    gbuf,
    acc,
    dsend,
    drecv,
    sbuf,
    rbuf_d,
    rbuf_f,
    rbuf_s,
    asem,
    psem,
    gsem,
    dssem,
    drsem,
    pssem,
    prsem,
    ssem,
    rsem,
    *gsems,
):
    x, y, core, first, second, partner = place()
    chip, first_chip, second_chip = chips(x, y, core)

    def part(r, c, half):
        q = panel(r, c // 2, c % 2)
        return out.at[
            q // PANELS,
            pl.ds(pl.multiple_of(half * HALF, 16), HALF),
            pl.ds(pl.multiple_of((q % PANELS) * TN, 128), TN),
        ]

    gather = Gather(gsems, part, lambda r: part(r, chip, core))

    def where_is(t):
        r, i = t // 4, t % 4
        ends = panel(r, jnp.where(i == 0, 1 - x, x), jnp.where(i == 0, 1 - y, y))
        mixed = (i == 1) | (i == 2)
        low = jnp.where(mixed, panel(r, 1 - x, y), ends)
        high = jnp.where(mixed, panel(r, x, 1 - y), ends)
        return low, jnp.where(i == 2, TH, 0), high, jnp.where(i == 1, 0, TH)

    def matrix(t):
        return where_is(t)[0] // PANELS

    def fresh(t):
        return matrix(t) != matrix(t - 1)

    def aload(t, mine):
        half = core if mine else 1 - core
        cols = pl.ds(pl.multiple_of(half * HALF, 128), HALF)
        return pltpu.make_async_copy(a.at[matrix(t), :, cols], abuf.at[int(mine)], asem.at[int(mine)])

    def apiece(mine, k):
        start, size = BLOCKS[k][0]
        half = core if mine else 1 - core
        cols = pl.ds(pl.multiple_of(half * HALF + start, 128), size)
        return pltpu.make_async_copy(a.at[0, :, cols], abuf.at[int(mine), :, pl.ds(start, size)], psem.at[int(mine), k])

    def gload(t):
        low, low_at, high, high_at = where_is(t)
        return [
            pltpu.make_async_copy(
                g.at[q // PANELS, :, pl.ds(pl.multiple_of((q % PANELS) * TN + at, 128), TH)],
                gbuf.at[t % 2, :, pl.ds(k * TH, TH)],
                gsem.at[t % 2, k],
            )
            for k, (q, at) in enumerate(((low, low_at), (high, high_at)))
        ]

    def partner_piece(k):
        (r0, rn), (c0, cn) = BLOCKS[k]
        at = (pl.ds(r0, rn), pl.ds(c0, cn))
        return remote(dsend.at[at], drecv.at[(0, *at)], pssem.at[k], prsem.at[k], partner)

    def partner_copy(t):
        return remote(dsend, drecv.at[t % 2], dssem, drsem.at[t % 2], partner)

    def hop(r, kind, at=(slice(None), slice(None))):
        depth, rbuf = ((2, rbuf_d), (3, rbuf_f), (3, rbuf_s))[kind]
        return remote(
            sbuf.at[(r % 2, kind, *at)],
            rbuf.at[(r % depth, *at)],
            ssem.at[r % 2, kind],
            rsem.at[r % depth, kind],
            second if kind == 2 else first,
        )

    def columns(k):
        return pl.ds(pl.multiple_of(k * TH, 128), TH)

    def half_hop(r, kind, k):
        return hop(r, kind, (slice(None), columns(k)))

    def rows(fn):
        def one(b, _):
            fn(pl.ds(pl.multiple_of(b * RB, 16), RB))
            return 0

        lax.fori_loop(0, HALF // RB, one, 0)

    def ready(r, kind):
        @pl.when(r >= 2)
        def _():
            hop(r - 2, kind).wait_send()

    def pass_on(r, k):
        if k == 0:
            hop(r, 0).wait_recv()
            if r >= 2:
                hop(r - 2, 2).wait_send()

        def put(s):
            total = acc[1, s, columns(k)] + rbuf_d[r % 2, s, columns(k)].astype(F32)
            sbuf[r % 2, 2, s, columns(k)] = total.astype(BF16)

        rows(put)
        half_hop(r, 2, k).start()

    def finish(r):
        hop(r, 1).wait_recv()
        hop(r, 2).wait_recv()
        done = part(r, chip, core)

        def add(s):
            total = acc[2, s, :] + rbuf_f[r % 3, s, :].astype(F32) + rbuf_s[r % 3, s, :].astype(F32)
            done[s, :] = total.astype(BF16)

        rows(add)

    def spread(r, kind):
        if kind == 0:
            gather.to_first(r).start()
            gather.across_own(r).start()
        elif kind == 1:
            gather.to_second(r).start()
        elif kind == 2:
            gather.to_second(r).wait_recv()
            gather.forward(r).start()
            gather.across(r, 1, second_chip).start()
        elif kind == 3:
            gather.to_first(r).wait_recv()
            gather.across(r, 2, first_chip).start()
        else:
            gather.forward(r).wait_recv()
            gather.across(r, 3, 3 - chip).start()

    actions = [(t, functools.partial(finish, r)) for r, t in enumerate(O_AT)]
    actions += [(t, functools.partial(pass_on, r, k)) for r, ts in enumerate(S_AT) for k, t in enumerate(ts)]
    actions += [(t, functools.partial(spread, r, kind)) for r, kind, t in AG_AT]
    actions.sort(key=lambda action: action[0])

    def act_at(t, now):
        for at, act in actions:
            if at < SLOTS and at % 1 == now:
                pl.when(t == int(at))(act)

    def dot(mine, t, at=(slice(None), slice(None))):
        return lax.dot_general(
            abuf[int(mine), :, at[0]], gbuf[t % 2, :, at[1]], (((0,), (0,)), ((), ())), preferred_element_type=F32
        )

    greet(first, second, partner)
    gload(0)[0].start()
    apiece(False, 0).start()
    apiece(True, 0).start()

    def block(k):
        return tuple(pl.ds(*b) for b in BLOCKS[k])

    def send_block(k):
        at = block(k)
        partner_piece(k).wait_recv()
        sbuf[(0, 0, *at)] = (acc[(0, *at)] + drecv[(0, *at)].astype(F32)).astype(BF16)
        hop(0, 0, at).start()

    for k in range(4):
        if k == 0:
            gload(0)[0].wait()
        if k == 2:
            gload(0)[1].wait()
        if k < 2:
            apiece(False, k).wait()
        if k == 0:
            apiece(False, 1).start()
            apiece(True, 1).start()
        dsend[block(k)] = dot(False, 0, block(k)).astype(BF16)
        if k == 0:
            pl.semaphore_wait(pltpu.get_barrier_semaphore(), 3)
        partner_piece(k).start()
        if k > 0:
            send_block(k - 1)
        if k < 2:
            apiece(True, k).wait()
        if k == 0:
            gload(0)[1].start()
        if k == 1:
            for load in gload(1):
                load.start()
        acc[(0, *block(k))] = dot(True, 0, block(k))
    send_block(3)
    for k in range(4):
        partner_piece(k).wait_send()

    def slot(t, _):
        r, i = t // 4, t % 4
        rp = r % 2
        more = t + 1 < SLOTS

        @pl.when(fresh(t))
        def _():
            aload(t, False).wait()

        for load in gload(t):
            load.wait()

        @pl.when(more)
        def _():
            for load in gload(t + 1):
                load.start()

        @pl.when(t >= 2)
        def _():
            partner_copy(t - 1).wait_send()

        dsend[...] = dot(False, t).astype(BF16)
        partner_copy(t).start()

        @pl.when(more & fresh(t + 1))
        def _():
            aload(t + 1, False).start()

        act_at(t, 0.5)

        @pl.when(fresh(t))
        def _():
            aload(t, True).wait()

        kept = jnp.where(i == 3, 2, 0)
        acc[kept] = dot(True, t)

        @pl.when(more & fresh(t + 1))
        def _():
            aload(t + 1, True).start()

        partner_copy(t).wait_recv()

        @pl.when(i == 0)
        def _():
            ready(r, 0)

            def put(s):
                sbuf[rp, 0, s, :] = (acc[0, s, :] + drecv[t % 2, s, :].astype(F32)).astype(BF16)

            rows(put)
            hop(r, 0).start()

        @pl.when(i == 3)
        def _():
            def put(s):
                acc[2, s, :] = acc[2, s, :] + drecv[t % 2, s, :].astype(F32)

            rows(put)

        @pl.when((i == 1) | (i == 2))
        def _():
            @pl.when(i == 1)
            def _():
                ready(r, 1)

            def put(s):
                mine, passed = columns(core), columns(1 - core)
                raw = acc[0, s, mine] + drecv[t % 2, s, mine].astype(F32)
                sbuf[rp, 1, s, columns(i - 1)] = raw.astype(BF16)
                acc[1, s, columns(i - 1)] = acc[0, s, passed] + drecv[t % 2, s, passed].astype(F32)

            rows(put)
            half_hop(r, 1, i - 1).start()

        act_at(t, 0)
        return 0

    lax.fori_loop(1, SLOTS, slot, 0)
    for at, act in actions:
        if at >= SLOTS:
            act()
    partner_copy(SLOTS - 1).wait_send()
    for r in (ROUNDS - 2, ROUNDS - 1):
        for kind in range(3):
            hop(r, kind).wait_send()

    def drain(r, _):
        gather.drain(r)
        return 0

    lax.fori_loop(0, ROUNDS, drain, 0)


def write_kernel(held, out, sem):
    copies = [pltpu.make_async_copy(held.at[n], out.at[n], sem.at[n]) for n in range(MATS)]
    for copy in copies:
        copy.start()
    for copy in copies:
        copy.wait()


def solution(mesh):
    any_space = pl.BlockSpec(memory_space=pl.ANY)
    vmem = pl.BlockSpec(memory_space=pltpu.VMEM)
    dma = pltpu.SemaphoreType.DMA

    def body(a, g):
        held = pl.pallas_call(
            sum_kernel,
            out_shape=pltpu.VMEM((MATS, D, FF), BF16),
            in_specs=[any_space] * 2,
            out_specs=vmem,
            scratch_shapes=[
                pltpu.VMEM((2, TOKENS, HALF), BF16),
                pltpu.VMEM((2, TOKENS, TN), BF16),
                pltpu.VMEM((3, HALF, TN), F32),
                pltpu.VMEM((HALF, TN), BF16),
                pltpu.VMEM((2, HALF, TN), BF16),
                pltpu.VMEM((2, 3, HALF, TN), BF16),
                pltpu.VMEM((2, HALF, TN), BF16),
                pltpu.VMEM((3, HALF, TN), BF16),
                pltpu.VMEM((3, HALF, TN), BF16),
                dma((2,)),
                dma((2, 2)),
                dma((2, 2)),
                dma,
                dma((2,)),
                dma((4,)),
                dma((4,)),
                dma((2, 3)),
                dma((3, 3)),
                dma((ROUNDS, 3)),
                dma((ROUNDS, 3)),
                dma((ROUNDS, 4)),
                dma((ROUNDS, 4)),
            ],
            compiler_params=pltpu.CompilerParams(
                collective_id=0, has_side_effects=True, vmem_limit_bytes=35_400_000
            ),
            name="sum_and_share",
        )(a[0], g[0])
        return pl.pallas_call(
            write_kernel,
            out_shape=jax.ShapeDtypeStruct((MATS, D, FF), BF16),
            in_specs=[vmem],
            out_specs=any_space,
            scratch_shapes=[dma((MATS,))],
            compiler_params=pltpu.CompilerParams(vmem_limit_bytes=16 * 2**20),
            name="write_out",
        )(held)

    return jax.shard_map(
        body, mesh=mesh, in_specs=P(("rep", "dp")), out_specs=P("rep"), check_vma=False
    )
```
